128 devices in a mesh: site: 128 (over y, z, x, core).
Axes of the slice: x: 4, y: 4, z: 4, core: 2. Of those that a mesh axis runs over, the one named last changes fastest.
Arguments:
- sites: float32 [128, 2, 12, 128, 128], P('site'), may hold values from -0.5 to 0.5
- sector_sizes: int32 [128, 12], P('site'), may hold values from 64 to 128, as said below
- charge_steps: int32 [128], P('site'), may hold values from 0 to 1
- kept_counts: int32 [128, 12], P('site'), may hold values from 64 to 128, as said below
- gates: float32 [128, 6], P('site'), may hold values from 0.4 to 1.2
- sketches: float32 [128, 12, 256, 128], P('site'), may hold values from -0.375 to 0.375
Outputs:
- new_sites: float32 [128, 2, 12, 128, 128], P('site')
- totals: float32 [2], replicated
The draws below stay inside these ranges and needn't reach their ends.
Inputs may be any that keep to these rules, and one draw needn't show every extreme that they name: `sector_sizes`: every sector holds at least 64 states; each bond has one sector of exactly 128 states. kept_counts[i, c] is at least 64 and at most sector_sizes[(i + 1) mod 128, c]; on each bond the sector of 128 states keeps all of them.
All inputs are finite; a program needn't handle non-finite values.
Results may differ from the reference program's by a relative error of at most 0.0003.
Values sent between devices are 32-bit elements; how exact they have to be, the bound alone decides.
No kernel may reach another device: no remote copies, remote signals or barrier semaphores. Data moves between devices by JAX's collectives and lax.ppermute only.
A program may use at most 64 MiB of HBM per device.

```python
import jax
import jax.numpy as jnp
from jax import lax

NSEC = 12
SMAX = 128
STEPS = 4
SITES = 128


def label_tables(key):
    sizes = jax.random.randint(jax.random.fold_in(key, 101), (SITES, NSEC), SMAX // 2, SMAX + 1)
    full_at = jax.random.randint(jax.random.fold_in(key, 102), (SITES,), 0, NSEC)
    sectors = jnp.arange(NSEC)[None, :]
    sizes = jnp.where(sectors == full_at[:, None], SMAX, sizes)
    following = jnp.roll(sizes, -1, axis=0)
    kept = jax.random.randint(jax.random.fold_in(key, 103), (SITES, NSEC), SMAX // 2, following + 1)
    whole_at = jnp.roll(full_at, -1)
    kept = jnp.where(sectors == whole_at[:, None], following, kept)
    return (sizes.astype(jnp.int32), kept.astype(jnp.int32))


def draw_sector_sizes(key, part):
    return label_tables(key)[0]


def draw_kept_counts(key, part):
    return label_tables(key)[1]


def touch_ends(values, rng, smallest, largest):
    longest = values.shape.index(max(values.shape))
    spots = []
    for shift in (0, 1):
        where = [jax.random.randint(jax.random.fold_in(rng, axis), (), 0, length) for axis, length in enumerate(values.shape)]
        where[longest] = (where[longest] + shift) % values.shape[longest]
        spots.append(tuple(where))
    return values.at[spots[0]].set(smallest).at[spots[1]].set(largest)


def level_of(own_key, shape, pieces, smallest, top_value):
    level, own = 1.0, jax.random.fold_in(own_key, 6)
    for position, shards_of in pieces:
        draws = jnp.exp(jax.random.uniform(jax.random.fold_in(own, position), (shards_of,), jnp.float32, smallest / len(pieces), top_value / len(pieces)))
        level = level * jnp.repeat(draws, shape[position] // shards_of).reshape([-1 if axis == position else 1 for axis in range(len(shape))])
    return level


def scatter_about(stream_key, extent, scale, most, cuts=(), kind=jnp.bfloat16):
    values = jax.random.normal(stream_key, extent, jnp.float32) * scale
    if len(cuts) > 0:
        values = level_of(stream_key, extent, cuts, -0.22, 0.18) * values
    return jnp.clip(values, min=-most, max=most).astype(kind)


def setup_inputs(seed: int = 0) -> dict:
    key_of = jax.random.split(jax.random.key(seed), 7)
    return {
        "sites": scatter_about(key_of[0], (SITES, 2, NSEC, SMAX, SMAX), SMAX ** -0.5, 0.5, ((0, 128),), jnp.float32),
        "sector_sizes": draw_sector_sizes(jax.random.fold_in(key_of[6], 71), 0),
        "charge_steps": touch_ends(jax.random.randint(key_of[2], (SITES,), 0, 2), jax.random.fold_in(key_of[2], 1), 0, 1).astype(jnp.int32),
        "kept_counts": draw_kept_counts(jax.random.fold_in(key_of[6], 71), 0),
        "gates": jnp.clip(0.4 + 0.800000042 * jax.random.uniform(key_of[4], (SITES, 6), jnp.float32) ** level_of(key_of[4], (SITES, 6), ((0, 128),), -0.2, 0.2), 0.4, 1.2),
        "sketches": scatter_about(key_of[5], (SITES, NSEC, 2 * SMAX, SMAX), (2 * SMAX) ** -0.5, 0.375, ((0, 128),), jnp.float32),
    }


def sector_index(count, shift, extra):
    return ((jnp.arange(count, dtype=jnp.int32) + extra - shift) % count).astype(jnp.int32)

def theta_blocks(left, right, shift, gate):
    count = left.shape[1]
    lower_mid = sector_index(count, shift, 0)
    upper_mid = sector_index(count, shift, 1)

    def product(first, second):
        return jnp.einsum('lam,lmb->lab', first, second, precision=lax.Precision.HIGHEST)
    zero_zero = product(left[0], right[0][lower_mid])
    zero_one = product(left[0], right[1][lower_mid])
    one_zero = product(left[1], right[0][upper_mid])
    one_one = product(left[1], right[1][upper_mid])
    mixed_up = gate[2] * zero_one + gate[3] * one_zero
    mixed_down = gate[4] * zero_one + gate[5] * one_zero
    return (gate[0] * zero_zero, mixed_up, mixed_down, gate[1] * one_one)

def split_sectors(blocks, middle, shift, sketch, kept):
    count = blocks[0].shape[0]
    width = blocks[0].shape[-1]
    top = ((middle + shift) % count).astype(jnp.int32)
    bottom = ((middle + shift - 1) % count).astype(jnp.int32)
    upper = jnp.concatenate([blocks[0][top], blocks[1][top]], axis=2)
    lower = jnp.concatenate([blocks[2][bottom], blocks[3][bottom]], axis=2)
    matrix = jnp.concatenate([upper, lower], axis=1)
    used = (jnp.arange(width, dtype=jnp.int32)[None, :] < kept[:, None]).astype(jnp.float32)
    sample = jnp.einsum('kij,kjs->kis', matrix, sketch * used[:, None, :], precision=lax.Precision.HIGHEST)
    gram = jnp.einsum('kis,kit->kst', sample, sample, precision=lax.Precision.HIGHEST)
    diag_sum = lax.optimization_barrier(jnp.sum(sample * sample, axis=(1, 2)))
    ridge = 0.001 * diag_sum / kept.astype(jnp.float32) + 1e-06
    identity = jnp.eye(width, dtype=jnp.float32)[None]
    gram = gram + identity * ridge[:, None, None] + identity * (1.0 - used)[:, None, :]
    factor = jnp.linalg.cholesky(gram)
    solved = jax.scipy.linalg.solve_triangular(factor, jnp.swapaxes(sample, 1, 2), lower=True)
    basis = jnp.swapaxes(solved, 1, 2)
    reduced = jnp.einsum('kis,kij->ksj', basis, matrix, precision=lax.Precision.HIGHEST)
    return (basis, reduced, jnp.sum(matrix * matrix), jnp.sum(reduced * reduced))

def rebuild(basis, reduced, shift, weight):
    count = basis.shape[0]
    width = basis.shape[2]
    left_new = jnp.stack([basis[sector_index(count, shift, 0), :width], basis[sector_index(count, shift, 1), width:]])
    right_new = jnp.stack([reduced[..., :width], reduced[..., width:]]) / jnp.sqrt(weight)
    return (left_new, right_new)

def bond_update(left, right, shift, gate, sketch, kept):
    blocks = theta_blocks(left, right, shift, gate)
    middle = jnp.arange(left.shape[1], dtype=jnp.int32)
    basis, reduced, total, weight = split_sectors(blocks, middle, shift, sketch, kept)
    left_new, right_new = rebuild(basis, reduced, shift, weight)
    return (left_new, right_new, 1.0 - weight / total, jnp.log(total))

def mask_sites(sites, sizes, steps):
    count = sites.shape[2]
    width = sites.shape[-1]
    following = jnp.roll(sizes, -1, axis=0)
    states = jnp.arange(width, dtype=jnp.int32)
    rows = states[None, None, :] < sizes[:, :, None]
    masks = []
    for phys in range(2):
        target = ((jnp.arange(count, dtype=jnp.int32)[None, :] + phys - steps[:, None]) % count).astype(jnp.int32)
        col_size = jnp.take_along_axis(following, target, axis=1)
        cols = states[None, None, :] < col_size[:, :, None]
        masks.append(rows[:, :, :, None] & cols[:, :, None, :])
    mask = jnp.stack(masks, axis=1)
    return sites * mask.astype(jnp.float32)

def reference(sites, sector_sizes, charge_steps, kept_counts, gates, sketches):
    state = mask_sites(sites, sector_sizes, charge_steps)
    chain = state.shape[0]
    discarded = jnp.zeros((), jnp.float32)
    log_total = jnp.zeros((), jnp.float32)
    for sweep in range(2 * STEPS):
        parity = sweep % 2
        pairs = chain // 2 - parity
        stop = parity + 2 * pairs
        items = (state[parity:stop:2], state[parity + 1:stop + 1:2], charge_steps[parity:stop:2], gates[parity:stop:2], sketches[parity:stop:2], kept_counts[parity:stop:2])

        def one_bond(item):
            return bond_update(item[0], item[1], item[2], item[3], item[4], item[5])
        new_left, new_right, lost, logs = lax.map(one_bond, items)
        state = state.at[parity:stop:2].set(new_left)
        state = state.at[parity + 1:stop + 1:2].set(new_right)
        discarded = discarded + jnp.sum(lost)
        log_total = log_total + jnp.sum(logs)
    return (state, jnp.stack([discarded, log_total]))
```

```python
import functools

import jax
import jax.numpy as jnp
from jax import lax
from jax.experimental import pallas as pl
from jax.experimental.pallas import tpu as pltpu
from jax.sharding import PartitionSpec as P

STEPS = 4
N = 128
NSEC = 12
HALF = 6
BLOCK = 2 * N
BULK = HALF * BLOCK
META = 32
F32 = jnp.float32
BF16 = jnp.bfloat16


def parts(x):
    one = x.astype(BF16)
    rest = x - one.astype(F32)
    two = rest.astype(BF16)
    three = (rest - two.astype(F32)).astype(BF16)
    return one, two, three


def dot(a, b, dims):
    return lax.dot_general(a, b, (dims, ((), ())), preferred_element_type=F32)


def product(a, b, dims):
    a1, a2, a3 = a
    b1, b2, b3 = b
    ca, cb = dims[0][0], dims[1][0]
    if a1.shape[ca] <= 128:
        low = dot(jnp.concatenate([a1, a3], ca), jnp.concatenate([b3, b1], cb), dims)
        pair = jnp.concatenate([a2, a1], ca)
        low = low + dot(pair, jnp.concatenate([b2, b2], cb), dims)
        return low + dot(pair, jnp.concatenate([b1, b1], cb), dims)
    out = dot(a1, b3, dims)
    out = out + dot(a3, b1, dims)
    out = out + dot(a2, b2, dims)
    out = out + dot(a1, b2, dims)
    out = out + dot(a2, b1, dims)
    return out + dot(a1, b1, dims)


NN = ((1,), (0,))
NT = ((1,), (1,))
TN = ((0,), (0,))


def row_of(x, m):
    return jnp.broadcast_to(x[m : m + 1, :], x.shape)


def eliminate(rows, start, lane, sub):
    columns = []
    for m in range(8):
        hit = lane == start + m
        columns.append(
            [
                jnp.broadcast_to(
                    jnp.sum(jnp.where(hit, r, 0.0), axis=1, keepdims=True), (8, N)
                )
                for r in rows
            ]
        )
    inside = (lane >= start) & (lane < start + 8)
    out = [jnp.where(inside, jnp.where(lane == start + sub, 1.0, 0.0), rows[0])]
    out += [jnp.where(inside, 0.0, r) for r in rows[1:]]
    scale = jnp.ones((8, N), F32)
    for m in range(8):
        inverse = lax.rsqrt(row_of(columns[m][0], m))
        lower = [c * inverse for c in columns[m]]
        lower[0] = jnp.where(sub > m, lower[0], 0.0)
        for j in range(m + 1, 8):
            factor = row_of(lower[0], j)
            for r in range(len(rows)):
                columns[j][r] = columns[j][r] - lower[r] * factor
        pivot = row_of(out[0], m) * inverse
        for r in range(len(rows)):
            out[r] = out[r] - lower[r] * pivot
        scale = jnp.where(sub == m, inverse, scale)
    out[0] = out[0] * scale
    return out


def invert_factors(gram):
    lane = lax.broadcasted_iota(jnp.int32, (8, N), 1)
    sub = lax.broadcasted_iota(jnp.int32, (8, N), 0)
    wide = lax.broadcasted_iota(jnp.int32, (N, N), 1)
    pair = lax.broadcasted_iota(jnp.int32, (16, N), 1)

    def body(index, carry):
        start = pl.multiple_of(index * 16, 16)
        inside = (wide >= start) & (wide < start + 16)
        for k in range(HALF):
            first = gram[k, pl.ds(start, 8), :]
            second = gram[k, pl.ds(start + 8, 8), :]
            first, second = eliminate([first, second], start, lane, sub)
            first = jnp.where((lane >= start + 8) & (lane < start + 16), 0.0, first)
            (second,) = eliminate([second], start + 8, lane, sub)
            both = jnp.concatenate([first, second], axis=0)
            z1, z2, z3 = parts(both)
            u1, u2, u3 = parts(jnp.where(pair >= start + 16, both, 0.0))
            change = dot(
                jnp.concatenate([u1, u1, u2, u2, u1, u3], 0),
                jnp.concatenate([z1, z2, z1, z2, z3, z1], 0),
                TN,
            )
            gram[k, :, :] = jnp.where(inside, 0.0, gram[k, :, :]) - change
            gram[k, pl.ds(start, 16), :] = both
        return carry

    lax.fori_loop(0, N // 16, body, 0)


def move(pairs, sem):
    copies = [
        pltpu.make_async_copy(source, target, sem.at[i])
        for i, (source, target) in enumerate(pairs)
    ]
    for c in copies:
        c.start()
    for c in copies:
        c.wait()


def sweep_kernel(
    parity,
    first_ref,
    scal,
    acc_in,
    keep,
    recv,
    chip,
    cross,
    sketch,
    acc_out,
    keep_out,
    send_out,
    chip_out,
    cross_out,
    left,
    left_sums,
    left_tail,
    right,
    matrix,
    up,
    down,
    sample,
    gram,
    red,
    bas,
    sem,
):
    core = scal[13]
    left_step = scal[14].astype(jnp.int32)
    right_step = scal[15].astype(jnp.int32)
    phantom = scal[12] > 0.5
    is_zero = core < 0.5
    first = first_ref[0] == 1
    left_kept = jnp.logical_or(first, is_zero if parity == 1 else jnp.logical_not(is_zero))
    left_chip = jnp.logical_or(first, is_zero)

    def load(left_from, right_from):
        move(
            [
                (
                    left_from.at[pl.ds(0, BULK)],
                    left.at[pl.ds(pl.multiple_of((1 - left_step) * BLOCK, BLOCK), BULK)],
                ),
                (left_from.at[pl.ds(BULK, 8)], left_sums),
                (
                    right_from.at[pl.ds(0, BULK)],
                    right.at[pl.ds(pl.multiple_of(right_step * BLOCK, BLOCK), BULK)],
                ),
            ],
            sem,
        )

    def load_edges(left_from, right_from):
        move(
            [
                (
                    left_from.at[pl.ds(0, BLOCK)],
                    left.at[pl.ds(pl.multiple_of(left_step * BULK, BLOCK), BLOCK)],
                ),
                (left_from.at[pl.ds(BLOCK, 8)], left_tail),
                (
                    right_from.at[pl.ds(0, BLOCK)],
                    right.at[pl.ds(pl.multiple_of((1 - right_step) * BULK, BLOCK), BLOCK)],
                ),
            ],
            sem,
        )

    pl.when(left_kept)(lambda: load(keep, recv))
    pl.when(jnp.logical_not(left_kept))(lambda: load(recv, keep))
    pl.when(left_chip)(lambda: load_edges(chip, cross))
    pl.when(jnp.logical_not(left_chip))(lambda: load_edges(cross, chip))

    sums = left_sums[...] + left_tail[...]
    weight_in = sums[0:1, :]
    total_in = sums[1:2, :]
    alpha = 1.0 / jnp.sqrt(weight_in)
    sub = lax.broadcasted_iota(jnp.int32, (8, N), 0)
    lost = 1.0 - weight_in / total_in
    acc_out[...] = acc_in[...] + jnp.where(
        sub == 0, lost, jnp.where(sub == 1, jnp.log(total_in), 0.0)
    )

    def finish(weight, total):
        tail = jnp.where(sub == 0, weight, jnp.where(sub == 1, total, 0.0))
        red[pl.ds(BULK, 8), :] = tail
        bas[pl.ds(BULK, 8), :] = tail

    @pl.when(phantom)
    def _():
        for k in range(HALF):
            at = k * BLOCK
            red[pl.ds(at, N), :] = right[pl.ds(at, N), :]
            red[pl.ds(at + N, N), :] = right[pl.ds(at + BLOCK + N, N), :]
            bas[pl.ds(at, N), :] = left[pl.ds(at + BLOCK, N), :] * alpha
            bas[pl.ds(at + N, N), :] = left[pl.ds(at + N, N), :] * alpha
        one = jnp.full((1, N), 1.0 - core, F32)
        finish(one, one)

    @pl.when(jnp.logical_not(phantom))
    def _():
        g = [scal[i] * alpha for i in range(6)]

        def thetas(k, carry):
            at = pl.multiple_of(k * BLOCK, BLOCK)
            a = jnp.concatenate(
                [left[pl.ds(at + BLOCK, N), :], left[pl.ds(at + N, N), :]], axis=0
            )
            b = jnp.concatenate(
                [right[pl.ds(at, N), :], right[pl.ds(at + BLOCK + N, N), :]], axis=1
            )
            theta = product(parts(a), parts(b), NN)
            matrix[k, 0:N, 0:N] = theta[0:N, 0:N] * g[0]
            matrix[k, N:BLOCK, N:BLOCK] = theta[N:BLOCK, N:BLOCK] * g[1]
            up[k + 1] = theta[0:N, N:BLOCK]
            down[k] = theta[N:BLOCK, 0:N]
            return carry

        lax.fori_loop(0, HALF, thetas, 0)
        up[0] = product(
            parts(left[pl.ds(0, N), :]), parts(right[pl.ds(N, N), :]), NN
        )
        down[HALF] = product(
            parts(left[pl.ds(BULK + N, N), :]), parts(right[pl.ds(BULK, N), :]), NN
        )

        row = lax.broadcasted_iota(jnp.int32, (N, N), 0)
        col = lax.broadcasted_iota(jnp.int32, (N, N), 1)

        def samples(k, total):
            matrix[k, 0:N, N:BLOCK] = up[k + 1] * g[2] + down[k + 1] * g[3]
            matrix[k, N:BLOCK, 0:N] = up[k] * g[4] + down[k] * g[5]
            m = matrix[k]
            squares = jnp.sum(m * m, axis=0, keepdims=True)
            s = product(parts(m), parts(sketch[k]), NN)
            sample[k] = s
            sp = parts(s)
            gr = product(sp, sp, TN)
            diag = jnp.sum(jnp.sum(s * s, axis=0, keepdims=True), axis=1, keepdims=True)
            kept = scal[6 + k]
            ridge = 0.001 * diag / kept + 1e-06
            extra = ridge + jnp.where(col.astype(F32) < kept, 0.0, 1.0)
            gram[k] = gr + jnp.where(row == col, extra, 0.0)
            return total + squares[:, 0:N] + squares[:, N:BLOCK]

        total = lax.fori_loop(0, HALF, samples, jnp.zeros((1, N), F32))
        invert_factors(gram)

        def split(k, weight):
            at = pl.multiple_of(k * BLOCK, BLOCK)
            x = jnp.where(col <= row, gram[k], 0.0)
            basis = product(parts(sample[k]), parts(x), NT)
            bas[pl.ds(at, BLOCK), :] = basis
            reduced = product(parts(basis), parts(matrix[k]), TN)
            red[pl.ds(at, N), :] = reduced[:, 0:N]
            red[pl.ds(at + N, N), :] = reduced[:, N:BLOCK]
            squares = jnp.sum(reduced * reduced, axis=0, keepdims=True)
            return weight + squares[:, 0:N] + squares[:, N:BLOCK]

        weight = lax.fori_loop(0, HALF, split, jnp.zeros((1, N), F32))
        finish(
            jnp.broadcast_to(jnp.sum(weight, axis=1, keepdims=True), (1, N)),
            jnp.broadcast_to(jnp.sum(total, axis=1, keepdims=True), (1, N)),
        )

    last = (HALF - 1) * BLOCK
    red_edge_at = pl.multiple_of((1 - right_step) * last, BLOCK)
    bas_edge_at = pl.multiple_of(left_step * last, BLOCK)

    def store(kept, sent):
        move([(kept, keep_out), (sent, send_out)], sem)

    def store_edges(red_edge, bas_edge):
        move(
            [
                (red.at[pl.ds(red_edge_at, BLOCK)], red_edge.at[pl.ds(0, BLOCK)]),
                (red.at[pl.ds(BULK, 8)], red_edge.at[pl.ds(BLOCK, 8)]),
                (bas.at[pl.ds(bas_edge_at, BLOCK)], bas_edge.at[pl.ds(0, BLOCK)]),
                (bas.at[pl.ds(BULK, 8)], bas_edge.at[pl.ds(BLOCK, 8)]),
            ],
            sem,
        )

    keeps_red = jnp.logical_not(is_zero) if parity == 1 else is_zero
    pl.when(keeps_red)(lambda: store(red, bas))
    pl.when(jnp.logical_not(keeps_red))(lambda: store(bas, red))
    pl.when(is_zero)(lambda: store_edges(cross_out, chip_out))
    pl.when(jnp.logical_not(is_zero))(lambda: store_edges(chip_out, cross_out))


VM = pl.BlockSpec(memory_space=pltpu.VMEM)
SM = pl.BlockSpec(memory_space=pltpu.SMEM)
HB = pl.BlockSpec(memory_space=pl.ANY)


def shape(*dims):
    return jax.ShapeDtypeStruct(dims, F32)


def sweep(parity, first, scal, acc, keep, recv, chip, cross, sketch):
    return pl.pallas_call(
        functools.partial(sweep_kernel, parity),
        out_shape=(
            shape(8, N),
            shape(BULK + 8, N),
            shape(BULK + 8, N),
            shape(BLOCK + 8, N),
            shape(BLOCK + 8, N),
        ),
        in_specs=[SM, SM, VM, HB, HB, HB, HB, VM],
        out_specs=(VM, HB, HB, HB, HB),
        scratch_shapes=[
            pltpu.VMEM((BLOCK + BULK, N), F32),
            pltpu.VMEM((8, N), F32),
            pltpu.VMEM((8, N), F32),
            pltpu.VMEM((BULK + BLOCK, N), F32),
            pltpu.VMEM((HALF, BLOCK, BLOCK), F32),
            pltpu.VMEM((HALF + 1, N, N), F32),
            pltpu.VMEM((HALF + 1, N, N), F32),
            pltpu.VMEM((HALF, BLOCK, N), F32),
            pltpu.VMEM((HALF, N, N), F32),
            pltpu.VMEM((BULK + 8, N), F32),
            pltpu.VMEM((BULK + 8, N), F32),
            pltpu.SemaphoreType.DMA((4,)),
        ],
        compiler_params=pltpu.CompilerParams(vmem_limit_bytes=56 * 1024 * 1024),
        cost_estimate=pl.CostEstimate(
            flops=4 * 10**8, bytes_accessed=4 * 10**6, transcendentals=0
        ),
        name="sweep",
    )(first, scal, acc, keep, recv, chip, cross, sketch)


HERE, THERE, AFTER, BEFORE = 0, 1, 2, 3


def wrap(index):
    return lax.rem(index + NSEC, NSEC)


def bond_scalars(scal, meta, bond, beyond, half, phantom, core):
    for i in range(6):
        scal[i] = meta[bond, i]
    for k in range(HALF):
        scal[6 + k] = meta[bond, 7 + half + k]
    scal[12] = jnp.where(phantom, 1.0, 0.0)
    scal[13] = jnp.where(core == 0, 0.0, 1.0)
    scal[14] = meta[bond, 6]
    scal[15] = meta[beyond, 6]


def mask_sketch(sketch, scal):
    col = lax.broadcasted_iota(jnp.int32, (BLOCK, N), 1).astype(F32)
    for k in range(HALF):
        sketch[k] = jnp.where(col < scal[6 + k], sketch[k], 0.0)


def start_kernel(
    pos, meta, site, other, mine, theirs, scal, odd_scal, left, right, chip, cross, sketch, sem
):
    position = pos[0]
    chain = pos[1]
    core = lax.rem(position, 2)
    half = core * HALF
    bond_scalars(scal, meta, HERE, THERE, half, False, core)
    phantom = jnp.where(core == 0, position == chain - 2, position == 1)
    odd = jnp.where(core == 0, THERE, BEFORE)
    beyond = jnp.where(core == 0, AFTER, HERE)
    bond_scalars(odd_scal, meta, odd, beyond, half, phantom, core)
    step = meta[HERE, 6].astype(jnp.int32)
    next_step = meta[THERE, 6].astype(jnp.int32)
    edge_left = wrap(half + jnp.where(step == 1, HALF, -1))
    edge_right = half + jnp.where(next_step == 1, -1, HALF)
    row = lax.broadcasted_iota(jnp.int32, (N, N), 0).astype(F32)
    col = lax.broadcasted_iota(jnp.int32, (N, N), 1).astype(F32)

    blocks = []
    for p in range(2):
        for k in range(HALF):
            at = k * BLOCK + p * N
            blocks.append((left, at, 0, p, half + k))
            blocks.append((right, at, 1, p, wrap(half + k - p + next_step)))
        blocks.append((chip, p * N, 0, p, edge_left))
        blocks.append((cross, p * N, 1, p, wrap(edge_right - p + next_step)))

    def load(pair, sketch_from):
        move(
            [(sketch_from.at[pl.ds(half, HALF)], sketch)]
            + [
                (pair[which].at[p, sector], ref.at[pl.ds(at, N)])
                for ref, at, which, p, sector in blocks
            ],
            sem,
        )

    pl.when(core == 0)(lambda: load((site, other), mine))
    pl.when(core == 1)(lambda: load((other, site), theirs))
    mask_sketch(sketch, scal)
    for ref, at, which, p, sector in blocks:
        target = wrap(sector + p - (next_step if which else step))
        rows = meta[THERE if which else HERE, 19 + sector]
        cols = meta[AFTER if which else THERE, 19 + target]
        ref[pl.ds(at, N), :] = jnp.where(
            (row < rows) & (col < cols), ref[pl.ds(at, N), :], 0.0
        )
    left[pl.ds(BULK, 8), :] = jnp.ones((8, N), F32)
    right[pl.ds(BULK, 8), :] = jnp.ones((8, N), F32)
    chip[pl.ds(BLOCK, 8), :] = jnp.zeros((8, N), F32)
    cross[pl.ds(BLOCK, 8), :] = jnp.zeros((8, N), F32)


def start(position, meta, site, other, mine, theirs):
    return pl.pallas_call(
        start_kernel,
        out_shape=(
            shape(16),
            shape(16),
            shape(BULK + 8, N),
            shape(BULK + 8, N),
            shape(BLOCK + 8, N),
            shape(BLOCK + 8, N),
            shape(HALF, BLOCK, N),
        ),
        in_specs=[SM, SM, HB, HB, HB, HB],
        out_specs=(SM, SM, VM, VM, VM, VM, VM),
        scratch_shapes=[pltpu.SemaphoreType.DMA((4 * HALF + 5,))],
        compiler_params=pltpu.CompilerParams(vmem_limit_bytes=24 * 1024 * 1024),
        name="start",
    )(position, meta, site, other, mine, theirs)


def odd_sketch_kernel(pos, odd_scal, theirs, behind, sketch, sem):
    core = lax.rem(pos[0], 2)

    def load(source):
        move([(source.at[pl.ds(core * HALF, HALF)], sketch)], sem)

    pl.when(core == 0)(lambda: load(theirs))
    pl.when(core == 1)(lambda: load(behind))
    mask_sketch(sketch, odd_scal)


def odd_sketch(position, odd_scal, theirs, behind):
    return pl.pallas_call(
        odd_sketch_kernel,
        out_shape=shape(HALF, BLOCK, N),
        in_specs=[SM, SM, HB, HB],
        out_specs=VM,
        scratch_shapes=[pltpu.SemaphoreType.DMA((1,))],
        compiler_params=pltpu.CompilerParams(vmem_limit_bytes=16 * 1024 * 1024),
        name="odd_sketch",
    )(position, odd_scal, theirs, behind)


def finish_kernel(pos, meta, acc, recv, swap, out, acc_out, sem):
    position = pos[0]
    core = lax.rem(position, 2)
    step = jnp.where(core == 0, 0.0, meta[THERE, 6]).astype(jnp.int32)
    sums = recv[pl.ds(BULK, 8), :] + swap[pl.ds(BULK, 8), :]
    weight = sums[0:1, :]
    total = sums[1:2, :]
    sub = lax.broadcasted_iota(jnp.int32, (8, N), 0)
    new = jnp.where(
        sub == 0, 1.0 - weight / total, jnp.where(sub == 1, jnp.log(total), 0.0)
    )
    acc_out[...] = jnp.where(core == 0, acc[...] + new, 0.0)

    @pl.when(core == 0)
    def _():
        alpha = 1.0 / jnp.sqrt(weight)
        recv[pl.ds(0, BULK), :] = recv[pl.ds(0, BULK), :] * alpha
        swap[pl.ds(0, BULK), :] = swap[pl.ds(0, BULK), :] * alpha
        pairs = []
        for k in range(HALF):
            for p in range(2):
                rows = pl.ds(k * BLOCK + p * N, N)
                pairs.append((recv.at[rows], out.at[p, k]))
                pairs.append((swap.at[rows], out.at[p, k + HALF]))
        move(pairs, sem)

    @pl.when(core == 1)
    def _():
        pairs = []
        for k in range(HALF):
            for p in range(2):
                rows = pl.ds(k * BLOCK + p * N, N)
                pairs.append((swap.at[rows], out.at[p, wrap(k - p + step)]))
                pairs.append((recv.at[rows], out.at[p, wrap(k + HALF - p + step)]))
        move(pairs, sem)


def finish(position, meta, acc, recv, swap):
    return pl.pallas_call(
        finish_kernel,
        out_shape=(shape(2, NSEC, N, N), shape(8, N)),
        in_specs=[SM, SM, VM, VM, VM],
        out_specs=(HB, VM),
        scratch_shapes=[pltpu.SemaphoreType.DMA((4 * HALF,))],
        compiler_params=pltpu.CompilerParams(vmem_limit_bytes=16 * 1024 * 1024),
        name="finish",
    )(position, meta, acc, recv, swap)


def everywhere(value, chain):
    stride = 1
    while stride < chain:
        size = 4 if (chain // stride) % 4 == 0 and stride > 1 else 2
        terms = [value]
        for turn in range(1, size):
            moves = [(i, i ^ (turn * stride)) for i in range(chain)]
            terms.append(lax.ppermute(value, "site", moves))
        while len(terms) > 1:
            terms = [a + b for a, b in zip(terms[0::2], terms[1::2])]
        value = terms[0]
        stride *= size
    return value


def body(sites, sector_sizes, charge_steps, kept_counts, gates, sketches):
    chain = lax.axis_size("site")
    here = lax.axis_index("site").astype(jnp.int32)
    position = jnp.stack([here, jnp.int32(chain)])
    core = here % 2
    chips = chain // 2

    def device(chip, core):
        return 2 * (chip % chips) + core

    swap = [(i, i ^ 1) for i in range(chain)]
    over = [(device(j, 0), device(j + 1, 1)) for j in range(chips)]
    over += [(device(j + 1, 1), device(j, 0)) for j in range(chips)]
    apart = [(device(j, 0), device(j - 1, 0)) for j in range(chips)]
    apart += [(device(j, 1), device(j + 1, 1)) for j in range(chips)]
    back = [(target, source) for source, target in apart]
    ahead = [(device(j, 1), device(j + 1, 1)) for j in range(chips)]

    row = jnp.concatenate(
        [
            gates[0],
            charge_steps.astype(F32),
            kept_counts[0].astype(F32),
            sector_sizes[0].astype(F32),
            jnp.zeros((1,), F32),
        ]
    )
    partner = lax.ppermute(row, "site", swap)
    along = lax.ppermute(row, "site", apart)
    across = lax.ppermute(along, "site", swap)
    after = jnp.where(core == 0, along, across)
    before = jnp.where(core == 0, across, along)
    meta = jnp.stack(
        [
            jnp.where(core == 0, row, partner),
            jnp.where(core == 0, partner, row),
            after,
            before,
        ]
    )
    site = sites[0]
    sketch = sketches[0]
    other = lax.ppermute(site, "site", swap)
    theirs = lax.ppermute(sketch, "site", swap)
    later, meta = lax.optimization_barrier((sketch, meta))
    behind = lax.ppermute(later, "site", ahead)
    scal, odd_scal, left, right, chip, cross, even = start(
        position, meta, site, other, sketch, theirs
    )
    odd = odd_sketch(position, odd_scal, theirs, behind)

    def spread(out, moves):
        acc, keep, send, chip, cross = out
        recv = lax.ppermute(send, "site", moves)
        cross = lax.ppermute(cross, "site", over)
        chip = lax.ppermute(chip, "site", swap)
        return acc, keep, recv, chip, cross

    def step(index, carry):
        first = jnp.where(index == 0, 1, 0).astype(jnp.int32)[None]
        none = jnp.zeros((1,), jnp.int32)
        carry = spread(sweep(0, first, scal, *carry, even), apart)
        return spread(sweep(1, none, scal_odd, *carry, odd), back)

    scal_odd = odd_scal
    carry = (jnp.zeros((8, N), F32), left, right, chip, cross)
    acc, keep, recv, chip, cross = lax.fori_loop(0, STEPS, step, carry)
    swapped = lax.ppermute(keep, "site", swap)
    out, acc = finish(position, meta, acc, recv, swapped)
    totals = everywhere(acc, chain)[0:2, 0]
    return (out[None], totals)


def solution(mesh):
    placed = (
        P("site", None, None, None, None),
        P("site", None),
        P("site"),
        P("site", None),
        P("site", None),
        P("site", None, None, None),
    )
    return jax.shard_map(
        body,
        mesh=mesh,
        in_specs=placed,
        out_specs=(P("site", None, None, None, None), P()),
        check_vma=False,
    )
```

```python
import functools

import jax
import jax.numpy as jnp
from jax import lax
from jax.experimental import pallas as pl
from jax.experimental.pallas import tpu as pltpu
from jax.sharding import PartitionSpec as P

STEPS = 4
N = 128
NSEC = 12
HALF = 6
BLOCK = 2 * N
BULK = HALF * BLOCK
META = 32
F32 = jnp.float32
BF16 = jnp.bfloat16


def parts(x):
    one = x.astype(BF16)
    rest = x - one.astype(F32)
    two = rest.astype(BF16)
    three = (rest - two.astype(F32)).astype(BF16)
    return one, two, three


def dot(a, b, dims):
    return lax.dot_general(a, b, (dims, ((), ())), preferred_element_type=F32)


def product(a, b, dims):
    a1, a2, a3 = a
    b1, b2, b3 = b
    ca, cb = dims[0][0], dims[1][0]
    if a1.shape[ca] <= 128:
        low = dot(jnp.concatenate([a1, a3], ca), jnp.concatenate([b3, b1], cb), dims)
        pair = jnp.concatenate([a2, a1], ca)
        low = low + dot(pair, jnp.concatenate([b2, b2], cb), dims)
        return low + dot(pair, jnp.concatenate([b1, b1], cb), dims)
    out = dot(a1, b3, dims)
    out = out + dot(a3, b1, dims)
    out = out + dot(a2, b2, dims)
    out = out + dot(a1, b2, dims)
    out = out + dot(a2, b1, dims)
    return out + dot(a1, b1, dims)


NN = ((1,), (0,))
NT = ((1,), (1,))
TN = ((0,), (0,))


def row_of(x, m):
    return jnp.broadcast_to(x[m : m + 1, :], x.shape)


def eliminate(groups, start, lane, sub):
    columns = [
        [
            [
                jnp.broadcast_to(
                    jnp.sum(jnp.where(lane == start + m, r, 0.0), axis=1, keepdims=True),
                    (8, N),
                )
                for r in rows
            ]
            for m in range(8)
        ]
        for rows in groups
    ]
    inside = (lane >= start) & (lane < start + 8)
    unit = jnp.where(lane == start + sub, 1.0, 0.0)
    outs = [
        [jnp.where(inside, unit, rows[0])] + [jnp.where(inside, 0.0, r) for r in rows[1:]]
        for rows in groups
    ]
    scales = [jnp.ones((8, N), F32) for _ in groups]
    for m in range(8):
        for g, out in enumerate(outs):
            column = columns[g]
            inverse = lax.rsqrt(row_of(column[m][0], m))
            lower = [c * inverse for c in column[m]]
            lower[0] = jnp.where(sub > m, lower[0], 0.0)
            for j in range(m + 1, 8):
                factor = row_of(lower[0], j)
                for r in range(len(out)):
                    column[j][r] = column[j][r] - lower[r] * factor
            pivot = row_of(out[0], m) * inverse
            for r in range(len(out)):
                out[r] = out[r] - lower[r] * pivot
            scales[g] = jnp.where(sub == m, inverse, scales[g])
    for out, scale in zip(outs, scales):
        out[0] = out[0] * scale
    return outs


def invert_factors(gram):
    lane = lax.broadcasted_iota(jnp.int32, (8, N), 1)
    sub = lax.broadcasted_iota(jnp.int32, (8, N), 0)
    wide = lax.broadcasted_iota(jnp.int32, (N, N), 1)
    pair = lax.broadcasted_iota(jnp.int32, (16, N), 1)

    def body(index, carry):
        start = pl.multiple_of(index * 16, 16)
        inside = (wide >= start) & (wide < start + 16)
        whole = [gram[k] for k in range(HALF)]
        rows = [
            [gram[k, pl.ds(start, 8), :], gram[k, pl.ds(start + 8, 8), :]]
            for k in range(HALF)
        ]
        rows = eliminate(rows, start, lane, sub)
        seconds = eliminate([[r[1]] for r in rows], start + 8, lane, sub)
        beyond = (lane >= start + 8) & (lane < start + 16)
        boths, changes = [], []
        for k in range(HALF):
            first = jnp.where(beyond, 0.0, rows[k][0])
            both = jnp.concatenate([first, seconds[k][0]], axis=0)
            z1, z2, z3 = parts(both)
            u1, u2, u3 = parts(jnp.where(pair >= start + 16, both, 0.0))
            changes.append(
                dot(
                    jnp.concatenate([u1, u1, u2, u2, u1, u3], 0),
                    jnp.concatenate([z1, z2, z1, z2, z3, z1], 0),
                    TN,
                )
            )
            boths.append(both)
        for k in range(HALF):
            gram[k] = jnp.where(inside, 0.0, whole[k]) - changes[k]
        for k in range(HALF):
            gram[k, pl.ds(start, 16), :] = boths[k]
        return carry

    lax.fori_loop(0, N // 16, body, 0)


def move(pairs, sem):
    copies = [
        pltpu.make_async_copy(source, target, sem.at[i])
        for i, (source, target) in enumerate(pairs)
    ]
    for c in copies:
        c.start()
    for c in copies:
        c.wait()


def sweep_kernel(
    parity,
    first_ref,
    scal,
    acc_in,
    keep,
    recv,
    chip,
    cross,
    sketch,
    acc_out,
    keep_out,
    send_out,
    chip_out,
    cross_out,
    left,
    right,
    matrix,
    up,
    down,
    sample,
    gram,
    red,
    bas,
):
    core = scal[13]
    left_step = scal[14].astype(jnp.int32)
    right_step = scal[15].astype(jnp.int32)
    phantom = scal[12] > 0.5
    is_zero = core < 0.5
    first = first_ref[0] == 1
    left_kept = jnp.logical_or(first, is_zero if parity == 1 else jnp.logical_not(is_zero))
    left_chip = jnp.logical_or(first, is_zero)

    def place(target, at, source, rows):
        target[pl.ds(pl.multiple_of(at, BLOCK), rows), :] = source[pl.ds(0, rows), :]

    def load(left_from, right_from):
        place(left, (1 - left_step) * BLOCK, left_from, BULK)
        place(right, right_step * BLOCK, right_from, BULK)

    def load_edges(left_from, right_from):
        place(left, left_step * BULK, left_from, BLOCK)
        place(right, (1 - right_step) * BULK, right_from, BLOCK)

    pl.when(left_kept)(lambda: load(keep, recv))
    pl.when(jnp.logical_not(left_kept))(lambda: load(recv, keep))
    pl.when(left_chip)(lambda: load_edges(chip, cross))
    pl.when(jnp.logical_not(left_chip))(lambda: load_edges(cross, chip))

    tail = pl.ds(BULK, 8)
    edge_tail = pl.ds(BLOCK, 8)
    sums = jnp.where(left_kept, keep[tail, :], recv[tail, :])
    sums = sums + jnp.where(left_chip, chip[edge_tail, :], cross[edge_tail, :])
    weight_in = sums[0:1, :]
    total_in = sums[1:2, :]
    alpha = 1.0 / jnp.sqrt(weight_in)
    sub = lax.broadcasted_iota(jnp.int32, (8, N), 0)
    lost = 1.0 - weight_in / total_in
    acc_out[...] = acc_in[...] + jnp.where(
        sub == 0, lost, jnp.where(sub == 1, jnp.log(total_in), 0.0)
    )

    def finish(weight, total):
        both = jnp.where(sub == 0, weight, jnp.where(sub == 1, total, 0.0))
        red[tail, :] = both
        bas[tail, :] = both

    def relabel():
        for k in range(HALF):
            at = k * BLOCK
            red[pl.ds(at, N), :] = right[pl.ds(at, N), :]
            red[pl.ds(at + N, N), :] = right[pl.ds(at + BLOCK + N, N), :]
            bas[pl.ds(at, N), :] = left[pl.ds(at + BLOCK, N), :] * alpha
            bas[pl.ds(at + N, N), :] = left[pl.ds(at + N, N), :] * alpha
        one = jnp.full((1, N), 1.0 - core, F32)
        finish(one, one)

    if parity == 1:
        pl.when(phantom)(relabel)

    @pl.when(jnp.logical_not(phantom))
    def _():
        g = [scal[i] * alpha for i in range(6)]

        def thetas(k, carry):
            at = pl.multiple_of(k * BLOCK, BLOCK)
            a = jnp.concatenate(
                [left[pl.ds(at + BLOCK, N), :], left[pl.ds(at + N, N), :]], axis=0
            )
            b = jnp.concatenate(
                [right[pl.ds(at, N), :], right[pl.ds(at + BLOCK + N, N), :]], axis=1
            )
            theta = product(parts(a), parts(b), NN)
            matrix[k, 0:N, 0:N] = theta[0:N, 0:N] * g[0]
            matrix[k, N:BLOCK, N:BLOCK] = theta[N:BLOCK, N:BLOCK] * g[1]
            up[k + 1] = theta[0:N, N:BLOCK]
            down[k] = theta[N:BLOCK, 0:N]
            return carry

        lax.fori_loop(0, HALF, thetas, 0, unroll=6)
        up[0] = product(
            parts(left[pl.ds(0, N), :]), parts(right[pl.ds(N, N), :]), NN
        )
        down[HALF] = product(
            parts(left[pl.ds(BULK + N, N), :]), parts(right[pl.ds(BULK, N), :]), NN
        )

        row = lax.broadcasted_iota(jnp.int32, (N, N), 0)
        col = lax.broadcasted_iota(jnp.int32, (N, N), 1)

        def samples(k, total):
            matrix[k, 0:N, N:BLOCK] = up[k + 1] * g[2] + down[k + 1] * g[3]
            matrix[k, N:BLOCK, 0:N] = up[k] * g[4] + down[k] * g[5]
            m = matrix[k]
            squares = jnp.sum(m * m, axis=0, keepdims=True)
            s = product(parts(m), parts(sketch[k]), NN)
            sample[k] = s
            sp = parts(s)
            gr = product(sp, sp, TN)
            diag = jnp.sum(jnp.sum(s * s, axis=0, keepdims=True), axis=1, keepdims=True)
            kept = scal[6 + k]
            ridge = 0.001 * diag / kept + 1e-06
            extra = ridge + jnp.where(col.astype(F32) < kept, 0.0, 1.0)
            gram[k] = gr + jnp.where(row == col, extra, 0.0)
            return total + squares[:, 0:N] + squares[:, N:BLOCK]

        total = lax.fori_loop(0, HALF, samples, jnp.zeros((1, N), F32), unroll=6)
        invert_factors(gram)

        def split(k, weight):
            at = pl.multiple_of(k * BLOCK, BLOCK)
            x = jnp.where(col <= row, gram[k], 0.0)
            basis = product(parts(sample[k]), parts(x), NT)
            bas[pl.ds(at, BLOCK), :] = basis
            reduced = product(parts(basis), parts(matrix[k]), TN)
            red[pl.ds(at, N), :] = reduced[:, 0:N]
            red[pl.ds(at + N, N), :] = reduced[:, N:BLOCK]
            squares = jnp.sum(reduced * reduced, axis=0, keepdims=True)
            return weight + squares[:, 0:N] + squares[:, N:BLOCK]

        weight = lax.fori_loop(0, HALF, split, jnp.zeros((1, N), F32), unroll=6)
        finish(
            jnp.broadcast_to(jnp.sum(weight, axis=1, keepdims=True), (1, N)),
            jnp.broadcast_to(jnp.sum(total, axis=1, keepdims=True), (1, N)),
        )

    last = (HALF - 1) * BLOCK
    red_edge_at = pl.multiple_of((1 - right_step) * last, BLOCK)
    bas_edge_at = pl.multiple_of(left_step * last, BLOCK)

    def store(kept, sent):
        keep_out[...] = kept[...]
        send_out[...] = sent[...]

    def store_edges(red_edge, bas_edge):
        red_edge[pl.ds(0, BLOCK), :] = red[pl.ds(red_edge_at, BLOCK), :]
        red_edge[edge_tail, :] = red[tail, :]
        bas_edge[pl.ds(0, BLOCK), :] = bas[pl.ds(bas_edge_at, BLOCK), :]
        bas_edge[edge_tail, :] = bas[tail, :]

    keeps_red = jnp.logical_not(is_zero) if parity == 1 else is_zero
    pl.when(keeps_red)(lambda: store(red, bas))
    pl.when(jnp.logical_not(keeps_red))(lambda: store(bas, red))
    pl.when(is_zero)(lambda: store_edges(cross_out, chip_out))
    pl.when(jnp.logical_not(is_zero))(lambda: store_edges(chip_out, cross_out))


VM = pl.BlockSpec(memory_space=pltpu.VMEM)
SM = pl.BlockSpec(memory_space=pltpu.SMEM)
HB = pl.BlockSpec(memory_space=pl.ANY)


def shape(*dims):
    return jax.ShapeDtypeStruct(dims, F32)


def sweep(parity, first, scal, acc, keep, recv, chip, cross, sketch):
    return pl.pallas_call(
        functools.partial(sweep_kernel, parity),
        out_shape=(
            shape(8, N),
            shape(BULK + 8, N),
            shape(BULK + 8, N),
            shape(BLOCK + 8, N),
            shape(BLOCK + 8, N),
        ),
        in_specs=[SM, SM, VM, VM, VM, VM, VM, VM],
        out_specs=(VM, VM, VM, VM, VM),
        scratch_shapes=[
            pltpu.VMEM((BLOCK + BULK, N), F32),
            pltpu.VMEM((BULK + BLOCK, N), F32),
            pltpu.VMEM((HALF, BLOCK, BLOCK), F32),
            pltpu.VMEM((HALF + 1, N, N), F32),
            pltpu.VMEM((HALF + 1, N, N), F32),
            pltpu.VMEM((HALF, BLOCK, N), F32),
            pltpu.VMEM((HALF, N, N), F32),
            pltpu.VMEM((BULK + 8, N), F32),
            pltpu.VMEM((BULK + 8, N), F32),
        ],
        compiler_params=pltpu.CompilerParams(vmem_limit_bytes=32 * 1024 * 1024),
        cost_estimate=pl.CostEstimate(
            flops=4 * 10**8, bytes_accessed=4 * 10**6, transcendentals=0
        ),
        name="sweep",
    )(first, scal, acc, keep, recv, chip, cross, sketch)


HERE, THERE, AFTER, BEFORE = 0, 1, 2, 3


def wrap(index):
    return lax.rem(index + NSEC, NSEC)


def bond_scalars(scal, meta, bond, beyond, half, phantom, core):
    for i in range(6):
        scal[i] = meta[bond, i]
    for k in range(HALF):
        scal[6 + k] = meta[bond, 7 + half + k]
    scal[12] = jnp.where(phantom, 1.0, 0.0)
    scal[13] = jnp.where(core == 0, 0.0, 1.0)
    scal[14] = meta[bond, 6]
    scal[15] = meta[beyond, 6]


def mask_sketch(sketch, scal):
    col = lax.broadcasted_iota(jnp.int32, (BLOCK, N), 1).astype(F32)
    for k in range(HALF):
        sketch[k] = jnp.where(col < scal[6 + k], sketch[k], 0.0)


def start_kernel(
    pos, meta, site, other, mine, theirs, scal, odd_scal, left, right, chip, cross, sketch, sem
):
    position = pos[0]
    chain = pos[1]
    core = lax.rem(position, 2)
    half = core * HALF
    bond_scalars(scal, meta, HERE, THERE, half, False, core)
    phantom = jnp.where(core == 0, position == chain - 2, position == 1)
    odd = jnp.where(core == 0, THERE, BEFORE)
    beyond = jnp.where(core == 0, AFTER, HERE)
    bond_scalars(odd_scal, meta, odd, beyond, half, phantom, core)
    step = meta[HERE, 6].astype(jnp.int32)
    next_step = meta[THERE, 6].astype(jnp.int32)
    edge_left = wrap(half + jnp.where(step == 1, HALF, -1))
    edge_right = half + jnp.where(next_step == 1, -1, HALF)
    row = lax.broadcasted_iota(jnp.int32, (N, N), 0).astype(F32)
    col = lax.broadcasted_iota(jnp.int32, (N, N), 1).astype(F32)

    blocks = []
    for p in range(2):
        for k in range(HALF):
            at = k * BLOCK + p * N
            blocks.append((left, at, 0, p, half + k))
            blocks.append((right, at, 1, p, wrap(half + k - p + next_step)))
        blocks.append((chip, p * N, 0, p, edge_left))
        blocks.append((cross, p * N, 1, p, wrap(edge_right - p + next_step)))

    def load(pair, sketch_from):
        move(
            [(sketch_from.at[pl.ds(half, HALF)], sketch)]
            + [
                (pair[which].at[p, sector], ref.at[pl.ds(at, N)])
                for ref, at, which, p, sector in blocks
            ],
            sem,
        )

    pl.when(core == 0)(lambda: load((site, other), mine))
    pl.when(core == 1)(lambda: load((other, site), theirs))
    mask_sketch(sketch, scal)
    for ref, at, which, p, sector in blocks:
        target = wrap(sector + p - (next_step if which else step))
        rows = meta[THERE if which else HERE, 19 + sector]
        cols = meta[AFTER if which else THERE, 19 + target]
        ref[pl.ds(at, N), :] = jnp.where(
            (row < rows) & (col < cols), ref[pl.ds(at, N), :], 0.0
        )
    left[pl.ds(BULK, 8), :] = jnp.ones((8, N), F32)
    right[pl.ds(BULK, 8), :] = jnp.ones((8, N), F32)
    chip[pl.ds(BLOCK, 8), :] = jnp.zeros((8, N), F32)
    cross[pl.ds(BLOCK, 8), :] = jnp.zeros((8, N), F32)


def start(position, meta, site, other, mine, theirs):
    return pl.pallas_call(
        start_kernel,
        out_shape=(
            shape(16),
            shape(16),
            shape(BULK + 8, N),
            shape(BULK + 8, N),
            shape(BLOCK + 8, N),
            shape(BLOCK + 8, N),
            shape(HALF, BLOCK, N),
        ),
        in_specs=[SM, SM, HB, HB, HB, HB],
        out_specs=(SM, SM, VM, VM, VM, VM, VM),
        scratch_shapes=[pltpu.SemaphoreType.DMA((4 * HALF + 5,))],
        compiler_params=pltpu.CompilerParams(vmem_limit_bytes=24 * 1024 * 1024),
        name="start",
    )(position, meta, site, other, mine, theirs)


def odd_sketch_kernel(pos, odd_scal, theirs, behind, sketch, sem):
    core = lax.rem(pos[0], 2)

    def load(source):
        move([(source, sketch)], sem)

    pl.when(core == 0)(lambda: load(theirs.at[pl.ds(0, HALF)]))
    pl.when(core == 1)(lambda: load(behind))
    mask_sketch(sketch, odd_scal)


def odd_sketch(position, odd_scal, theirs, behind):
    return pl.pallas_call(
        odd_sketch_kernel,
        out_shape=shape(HALF, BLOCK, N),
        in_specs=[SM, SM, HB, HB],
        out_specs=VM,
        scratch_shapes=[pltpu.SemaphoreType.DMA((1,))],
        compiler_params=pltpu.CompilerParams(vmem_limit_bytes=16 * 1024 * 1024),
        name="odd_sketch",
    )(position, odd_scal, theirs, behind)


def finish_kernel(pos, meta, recv, swap, out, sem):
    position = pos[0]
    core = lax.rem(position, 2)
    step = jnp.where(core == 0, 0.0, meta[THERE, 6]).astype(jnp.int32)
    sums = recv[pl.ds(BULK, 8), :] + swap[pl.ds(BULK, 8), :]
    weight = sums[0:1, :]

    @pl.when(core == 0)
    def _():
        alpha = 1.0 / jnp.sqrt(weight)
        recv[pl.ds(0, BULK), :] = recv[pl.ds(0, BULK), :] * alpha
        swap[pl.ds(0, BULK), :] = swap[pl.ds(0, BULK), :] * alpha
        pairs = []
        for k in range(HALF):
            for p in range(2):
                rows = pl.ds(k * BLOCK + p * N, N)
                pairs.append((recv.at[rows], out.at[p, k]))
                pairs.append((swap.at[rows], out.at[p, k + HALF]))
        move(pairs, sem)

    @pl.when(core == 1)
    def _():
        pairs = []
        for k in range(HALF):
            for p in range(2):
                rows = pl.ds(k * BLOCK + p * N, N)
                pairs.append((swap.at[rows], out.at[p, wrap(k - p + step)]))
                pairs.append((recv.at[rows], out.at[p, wrap(k + HALF - p + step)]))
        move(pairs, sem)


def finish(position, meta, recv, swap):
    return pl.pallas_call(
        finish_kernel,
        out_shape=shape(2, NSEC, N, N),
        in_specs=[SM, SM, VM, VM],
        out_specs=HB,
        scratch_shapes=[pltpu.SemaphoreType.DMA((4 * HALF,))],
        compiler_params=pltpu.CompilerParams(vmem_limit_bytes=16 * 1024 * 1024),
        name="finish",
    )(position, meta, recv, swap)


def everywhere(value, chain):
    stride = 1
    while stride < chain:
        size = 4 if (chain // stride) % 4 == 0 and stride > 1 else 2
        terms = [value]
        for turn in range(1, size):
            moves = [(i, i ^ (turn * stride)) for i in range(chain)]
            terms.append(lax.ppermute(value, "site", moves))
        while len(terms) > 1:
            terms = [a + b for a, b in zip(terms[0::2], terms[1::2])]
        value = terms[0]
        stride *= size
    return value


def body(sites, sector_sizes, charge_steps, kept_counts, gates, sketches):
    chain = lax.axis_size("site")
    here = lax.axis_index("site").astype(jnp.int32)
    position = jnp.stack([here, jnp.int32(chain)])
    core = here % 2
    chips = chain // 2

    def device(chip, core):
        return 2 * (chip % chips) + core

    swap = [(i, i ^ 1) for i in range(chain)]
    over = [(device(j, 0), device(j + 1, 1)) for j in range(chips)]
    over += [(device(j + 1, 1), device(j, 0)) for j in range(chips)]
    apart = [(device(j, 0), device(j - 1, 0)) for j in range(chips)]
    apart += [(device(j, 1), device(j + 1, 1)) for j in range(chips)]
    back = [(target, source) for source, target in apart]
    slant = [(device(j + 1, 0), device(j, 1)) for j in range(chips)]
    slant += [(device(j, 1), device(j + 1, 0)) for j in range(chips)]
    ahead = [(device(j, 1), device(j + 1, 1)) for j in range(chips)]

    row = jnp.concatenate(
        [
            gates[0],
            charge_steps.astype(F32),
            kept_counts[0].astype(F32),
            sector_sizes[0].astype(F32),
            jnp.zeros((1,), F32),
        ]
    )
    partner = lax.ppermute(row, "site", swap)
    along = lax.ppermute(row, "site", apart)
    across = lax.ppermute(row, "site", slant)
    meta = jnp.stack(
        [
            jnp.where(core == 0, row, partner),
            jnp.where(core == 0, partner, row),
            jnp.where(core == 0, along, across),
            jnp.where(core == 0, across, along),
        ]
    )
    site = sites[0]
    sketch = sketches[0]
    other = lax.ppermute(site, "site", swap)
    theirs = lax.ppermute(sketch, "site", swap)
    later, meta = lax.optimization_barrier((sketch[HALF:], meta))
    behind = lax.ppermute(later, "site", ahead)
    scal, odd_scal, left, right, chip, cross, even = start(
        position, meta, site, other, sketch, theirs
    )
    odd = odd_sketch(position, odd_scal, theirs, behind)

    def spread(out, moves):
        acc, keep, send, chip, cross = out
        recv = lax.ppermute(send, "site", moves)
        cross = lax.ppermute(cross, "site", over)
        chip = lax.ppermute(chip, "site", swap)
        return acc, keep, recv, chip, cross

    none = jnp.zeros((1,), jnp.int32)

    def even_sweep(first, carry):
        return spread(sweep(0, first, scal, *carry, even), apart)

    def odd_sweep(carry):
        return spread(sweep(1, none, odd_scal, *carry, odd), back)

    carry = (jnp.zeros((8, N), F32), left, right, chip, cross)
    carry = even_sweep(none + 1, carry)
    carry = lax.fori_loop(
        0, STEPS - 1, lambda _, carry: even_sweep(none, odd_sweep(carry)), carry
    )
    acc, keep, send, chip, cross = sweep(1, none, odd_scal, *carry, odd)
    tail = keep[BULK:]
    met = tail + lax.ppermute(tail, "site", over)
    weight, total = met[0:1], met[1:2]
    last = jnp.concatenate([1.0 - weight / total, jnp.log(total), met[2:]], axis=0)
    acc = jnp.where(core == 0, acc + last, 0.0)
    totals = everywhere(acc, chain)[0:2, 0]
    recv = lax.ppermute(send, "site", back)
    swapped = lax.ppermute(keep, "site", swap)
    out = finish(position, meta, recv, swapped)
    return (out[None], totals)


def solution(mesh):
    placed = (
        P("site", None, None, None, None),
        P("site", None),
        P("site"),
        P("site", None),
        P("site", None),
        P("site", None, None, None),
    )
    return jax.shard_map(
        body,
        mesh=mesh,
        in_specs=placed,
        out_specs=(P("site", None, None, None, None), P()),
        check_vma=False,
    )
```

```python
import functools

import jax
import jax.numpy as jnp
from jax import lax
from jax.experimental import pallas as pl
from jax.experimental.pallas import tpu as pltpu
from jax.sharding import PartitionSpec as P

STEPS = 4
N = 128
NSEC = 12
HALF = 6
BLOCK = 2 * N
BULK = HALF * BLOCK
META = 32
F32 = jnp.float32
BF16 = jnp.bfloat16


def parts(x):
    one = x.astype(BF16)
    rest = x - one.astype(F32)
    two = rest.astype(BF16)
    three = (rest - two.astype(F32)).astype(BF16)
    return one, two, three


def dot(a, b, dims):
    return lax.dot_general(a, b, (dims, ((), ())), preferred_element_type=F32)


def product(a, b, dims):
    a1, a2, a3 = a
    b1, b2, b3 = b
    ca, cb = dims[0][0], dims[1][0]
    if a1.shape[ca] <= 128:
        low = dot(jnp.concatenate([a1, a3], ca), jnp.concatenate([b3, b1], cb), dims)
        pair = jnp.concatenate([a2, a1], ca)
        low = low + dot(pair, jnp.concatenate([b2, b2], cb), dims)
        return low + dot(pair, jnp.concatenate([b1, b1], cb), dims)
    cn = 1 - cb
    if b1.shape[cn] <= 128:
        both = jnp.concatenate([b1, b2], cn)
        wide = dot(a2, both, dims)
        wide = wide + dot(a1, both, dims)
        out = dot(a1, b3, dims)
        out = out + dot(a3, b1, dims)
        return out + wide[:, 128:] + wide[:, :128]
    out = dot(a1, b3, dims)
    out = out + dot(a3, b1, dims)
    out = out + dot(a2, b2, dims)
    out = out + dot(a1, b2, dims)
    out = out + dot(a2, b1, dims)
    return out + dot(a1, b1, dims)


NN = ((1,), (0,))
NT = ((1,), (1,))
TN = ((0,), (0,))


def row_of(x, m):
    return jnp.broadcast_to(x[m : m + 1, :], x.shape)


def eliminate(groups, start, lane, sub):
    columns = [
        [
            [
                jnp.broadcast_to(
                    jnp.sum(jnp.where(lane == start + m, r, 0.0), axis=1, keepdims=True),
                    (8, N),
                )
                for r in rows
            ]
            for m in range(8)
        ]
        for rows in groups
    ]
    inside = (lane >= start) & (lane < start + 8)
    unit = jnp.where(lane == start + sub, 1.0, 0.0)
    outs = [
        [jnp.where(inside, unit, rows[0])] + [jnp.where(inside, 0.0, r) for r in rows[1:]]
        for rows in groups
    ]
    scales = [jnp.ones((8, N), F32) for _ in groups]
    for m in range(8):
        for g, out in enumerate(outs):
            column = columns[g]
            inverse = lax.rsqrt(row_of(column[m][0], m))
            lower = [c * inverse for c in column[m]]
            lower[0] = jnp.where(sub > m, lower[0], 0.0)
            for j in range(m + 1, 8):
                factor = row_of(lower[0], j)
                for r in range(len(out)):
                    column[j][r] = column[j][r] - lower[r] * factor
            pivot = row_of(out[0], m) * inverse
            for r in range(len(out)):
                out[r] = out[r] - lower[r] * pivot
            scales[g] = jnp.where(sub == m, inverse, scales[g])
    for out, scale in zip(outs, scales):
        out[0] = out[0] * scale
    return outs


def invert_factors(gram):
    lane = lax.broadcasted_iota(jnp.int32, (8, N), 1)
    sub = lax.broadcasted_iota(jnp.int32, (8, N), 0)
    wide = lax.broadcasted_iota(jnp.int32, (N, N), 1)
    pair = lax.broadcasted_iota(jnp.int32, (16, N), 1)

    def body(index, carry):
        start = pl.multiple_of(index * 16, 16)
        inside = (wide >= start) & (wide < start + 16)
        whole = [gram[k] for k in range(HALF)]
        rows = [
            [gram[k, pl.ds(start, 8), :], gram[k, pl.ds(start + 8, 8), :]]
            for k in range(HALF)
        ]
        rows = eliminate(rows, start, lane, sub)
        seconds = eliminate([[r[1]] for r in rows], start + 8, lane, sub)
        beyond = (lane >= start + 8) & (lane < start + 16)
        boths, changes = [], []
        for k in range(HALF):
            first = jnp.where(beyond, 0.0, rows[k][0])
            both = jnp.concatenate([first, seconds[k][0]], axis=0)
            z1, z2, z3 = parts(both)
            u1, u2, u3 = parts(jnp.where(pair >= start + 16, both, 0.0))
            changes.append(
                dot(
                    jnp.concatenate([u1, u1, u2, u2, u1, u3], 0),
                    jnp.concatenate([z1, z2, z1, z2, z3, z1], 0),
                    TN,
                )
            )
            boths.append(both)
        for k in range(HALF):
            gram[k] = jnp.where(inside, 0.0, whole[k]) - changes[k]
        for k in range(HALF):
            gram[k, pl.ds(start, 16), :] = boths[k]
        return carry

    lax.fori_loop(0, N // 16, body, 0)


def move(pairs, sem):
    copies = [
        pltpu.make_async_copy(source, target, sem.at[i])
        for i, (source, target) in enumerate(pairs)
    ]
    for c in copies:
        c.start()
    for c in copies:
        c.wait()


def sweep_kernel(
    parity,
    first_ref,
    scal,
    acc_in,
    keep,
    recv,
    chip,
    cross,
    sketch,
    acc_out,
    keep_out,
    send_out,
    chip_out,
    cross_out,
    left,
    right,
    matrix,
    up,
    down,
    sample,
    gram,
    red,
    bas,
):
    core = scal[13]
    left_step = scal[14].astype(jnp.int32)
    right_step = scal[15].astype(jnp.int32)
    phantom = scal[12] > 0.5
    is_zero = core < 0.5
    first = first_ref[0] == 1
    left_kept = jnp.logical_or(first, is_zero if parity == 1 else jnp.logical_not(is_zero))
    left_chip = jnp.logical_or(first, is_zero)

    def place(target, at, source, rows):
        target[pl.ds(pl.multiple_of(at, BLOCK), rows), :] = source[pl.ds(0, rows), :]

    def load(left_from, right_from):
        place(left, (1 - left_step) * BLOCK, left_from, BULK)
        place(right, right_step * BLOCK, right_from, BULK)

    def load_edges(left_from, right_from):
        place(left, left_step * BULK, left_from, BLOCK)
        place(right, (1 - right_step) * BULK, right_from, BLOCK)

    pl.when(left_kept)(lambda: load(keep, recv))
    pl.when(jnp.logical_not(left_kept))(lambda: load(recv, keep))
    pl.when(left_chip)(lambda: load_edges(chip, cross))
    pl.when(jnp.logical_not(left_chip))(lambda: load_edges(cross, chip))

    tail = pl.ds(BULK, 8)
    edge_tail = pl.ds(BLOCK, 8)
    sums = jnp.where(left_kept, keep[tail, :], recv[tail, :])
    sums = sums + jnp.where(left_chip, chip[edge_tail, :], cross[edge_tail, :])
    weight_in = sums[0:1, :]
    total_in = sums[1:2, :]
    alpha = 1.0 / jnp.sqrt(weight_in)
    sub = lax.broadcasted_iota(jnp.int32, (8, N), 0)
    lost = 1.0 - weight_in / total_in
    acc_out[...] = acc_in[...] + jnp.where(
        sub == 0, lost, jnp.where(sub == 1, jnp.log(total_in), 0.0)
    )

    def finish(weight, total):
        both = jnp.where(sub == 0, weight, jnp.where(sub == 1, total, 0.0))
        red[tail, :] = both
        bas[tail, :] = both

    def relabel():
        for k in range(HALF):
            at = k * BLOCK
            red[pl.ds(at, N), :] = right[pl.ds(at, N), :]
            red[pl.ds(at + N, N), :] = right[pl.ds(at + BLOCK + N, N), :]
            bas[pl.ds(at, N), :] = left[pl.ds(at + BLOCK, N), :] * alpha
            bas[pl.ds(at + N, N), :] = left[pl.ds(at + N, N), :] * alpha
        one = jnp.full((1, N), 1.0 - core, F32)
        finish(one, one)

    if parity == 1:
        pl.when(phantom)(relabel)

    @pl.when(jnp.logical_not(phantom))
    def _():
        g = [scal[i] * alpha for i in range(6)]

        def thetas(k, carry):
            at = pl.multiple_of(k * BLOCK, BLOCK)
            a = jnp.concatenate(
                [left[pl.ds(at + BLOCK, N), :], left[pl.ds(at + N, N), :]], axis=0
            )
            b = jnp.concatenate(
                [right[pl.ds(at, N), :], right[pl.ds(at + BLOCK + N, N), :]], axis=1
            )
            theta = product(parts(a), parts(b), NN)
            matrix[k, 0:N, 0:N] = theta[0:N, 0:N] * g[0]
            matrix[k, N:BLOCK, N:BLOCK] = theta[N:BLOCK, N:BLOCK] * g[1]
            up[k + 1] = theta[0:N, N:BLOCK]
            down[k] = theta[N:BLOCK, 0:N]
            return carry

        lax.fori_loop(0, HALF, thetas, 0, unroll=6)
        up[0] = product(
            parts(left[pl.ds(0, N), :]), parts(right[pl.ds(N, N), :]), NN
        )
        down[HALF] = product(
            parts(left[pl.ds(BULK + N, N), :]), parts(right[pl.ds(BULK, N), :]), NN
        )

        row = lax.broadcasted_iota(jnp.int32, (N, N), 0)
        col = lax.broadcasted_iota(jnp.int32, (N, N), 1)

        def samples(k, total):
            matrix[k, 0:N, N:BLOCK] = up[k + 1] * g[2] + down[k + 1] * g[3]
            matrix[k, N:BLOCK, 0:N] = up[k] * g[4] + down[k] * g[5]
            m = matrix[k]
            squares = jnp.sum(m * m, axis=0, keepdims=True)
            s = product(parts(m), parts(sketch[k]), NN)
            sample[k] = s
            sp = parts(s)
            gr = product(sp, sp, TN)
            diag = jnp.sum(jnp.sum(s * s, axis=0, keepdims=True), axis=1, keepdims=True)
            kept = scal[6 + k]
            ridge = 0.001 * diag / kept + 1e-06
            extra = ridge + jnp.where(col.astype(F32) < kept, 0.0, 1.0)
            gram[k] = gr + jnp.where(row == col, extra, 0.0)
            return total + squares[:, 0:N] + squares[:, N:BLOCK]

        total = lax.fori_loop(0, HALF, samples, jnp.zeros((1, N), F32), unroll=6)
        invert_factors(gram)

        def split(k, weight):
            at = pl.multiple_of(k * BLOCK, BLOCK)
            x = jnp.where(col <= row, gram[k], 0.0)
            basis = product(parts(sample[k]), parts(x), NT)
            bas[pl.ds(at, BLOCK), :] = basis
            reduced = product(parts(basis), parts(matrix[k]), TN)
            red[pl.ds(at, N), :] = reduced[:, 0:N]
            red[pl.ds(at + N, N), :] = reduced[:, N:BLOCK]
            squares = jnp.sum(reduced * reduced, axis=0, keepdims=True)
            return weight + squares[:, 0:N] + squares[:, N:BLOCK]

        weight = lax.fori_loop(0, HALF, split, jnp.zeros((1, N), F32), unroll=6)
        finish(
            jnp.broadcast_to(jnp.sum(weight, axis=1, keepdims=True), (1, N)),
            jnp.broadcast_to(jnp.sum(total, axis=1, keepdims=True), (1, N)),
        )

    last = (HALF - 1) * BLOCK
    red_edge_at = pl.multiple_of((1 - right_step) * last, BLOCK)
    bas_edge_at = pl.multiple_of(left_step * last, BLOCK)

    def store(kept, sent):
        keep_out[...] = kept[...]
        send_out[...] = sent[...]

    def store_edges(red_edge, bas_edge):
        red_edge[pl.ds(0, BLOCK), :] = red[pl.ds(red_edge_at, BLOCK), :]
        red_edge[edge_tail, :] = red[tail, :]
        bas_edge[pl.ds(0, BLOCK), :] = bas[pl.ds(bas_edge_at, BLOCK), :]
        bas_edge[edge_tail, :] = bas[tail, :]

    keeps_red = jnp.logical_not(is_zero) if parity == 1 else is_zero
    pl.when(keeps_red)(lambda: store(red, bas))
    pl.when(jnp.logical_not(keeps_red))(lambda: store(bas, red))
    pl.when(is_zero)(lambda: store_edges(cross_out, chip_out))
    pl.when(jnp.logical_not(is_zero))(lambda: store_edges(chip_out, cross_out))


VM = pl.BlockSpec(memory_space=pltpu.VMEM)
SM = pl.BlockSpec(memory_space=pltpu.SMEM)
HB = pl.BlockSpec(memory_space=pl.ANY)


def shape(*dims):
    return jax.ShapeDtypeStruct(dims, F32)


def sweep(parity, first, scal, acc, keep, recv, chip, cross, sketch):
    return pl.pallas_call(
        functools.partial(sweep_kernel, parity),
        out_shape=(
            shape(8, N),
            shape(BULK + 8, N),
            shape(BULK + 8, N),
            shape(BLOCK + 8, N),
            shape(BLOCK + 8, N),
        ),
        in_specs=[SM, SM, VM, VM, VM, VM, VM, VM],
        out_specs=(VM, VM, VM, VM, VM),
        scratch_shapes=[
            pltpu.VMEM((BLOCK + BULK, N), F32),
            pltpu.VMEM((BULK + BLOCK, N), F32),
            pltpu.VMEM((HALF, BLOCK, BLOCK), F32),
            pltpu.VMEM((HALF + 1, N, N), F32),
            pltpu.VMEM((HALF + 1, N, N), F32),
            pltpu.VMEM((HALF, BLOCK, N), F32),
            pltpu.VMEM((HALF, N, N), F32),
            pltpu.VMEM((BULK + 8, N), F32),
            pltpu.VMEM((BULK + 8, N), F32),
        ],
        compiler_params=pltpu.CompilerParams(vmem_limit_bytes=32 * 1024 * 1024),
        cost_estimate=pl.CostEstimate(
            flops=4 * 10**8, bytes_accessed=4 * 10**6, transcendentals=0
        ),
        name="sweep",
    )(first, scal, acc, keep, recv, chip, cross, sketch)


HERE, THERE, AFTER, BEFORE = 0, 1, 2, 3


def wrap(index):
    return lax.rem(index + NSEC, NSEC)


def bond_scalars(scal, meta, bond, beyond, half, phantom, core):
    for i in range(6):
        scal[i] = meta[bond, i]
    for k in range(HALF):
        scal[6 + k] = meta[bond, 7 + half + k]
    scal[12] = jnp.where(phantom, 1.0, 0.0)
    scal[13] = jnp.where(core == 0, 0.0, 1.0)
    scal[14] = meta[bond, 6]
    scal[15] = meta[beyond, 6]


def mask_sketch(sketch, scal):
    col = lax.broadcasted_iota(jnp.int32, (BLOCK, N), 1).astype(F32)
    for k in range(HALF):
        sketch[k] = jnp.where(col < scal[6 + k], sketch[k], 0.0)


def start_kernel(
    pos, meta, site, other, mine, theirs, scal, odd_scal, left, right, chip, cross, sketch, sem
):
    position = pos[0]
    chain = pos[1]
    core = lax.rem(position, 2)
    half = core * HALF
    bond_scalars(scal, meta, HERE, THERE, half, False, core)
    phantom = jnp.where(core == 0, position == chain - 2, position == 1)
    odd = jnp.where(core == 0, THERE, BEFORE)
    beyond = jnp.where(core == 0, AFTER, HERE)
    bond_scalars(odd_scal, meta, odd, beyond, half, phantom, core)
    step = meta[HERE, 6].astype(jnp.int32)
    next_step = meta[THERE, 6].astype(jnp.int32)
    edge_left = wrap(half + jnp.where(step == 1, HALF, -1))
    edge_right = half + jnp.where(next_step == 1, -1, HALF)
    row = lax.broadcasted_iota(jnp.int32, (N, N), 0).astype(F32)
    col = lax.broadcasted_iota(jnp.int32, (N, N), 1).astype(F32)

    blocks = []
    for p in range(2):
        for k in range(HALF):
            at = k * BLOCK + p * N
            blocks.append((left, at, 0, p, half + k))
            blocks.append((right, at, 1, p, wrap(half + k - p + next_step)))
        blocks.append((chip, p * N, 0, p, edge_left))
        blocks.append((cross, p * N, 1, p, wrap(edge_right - p + next_step)))

    def load(pair, sketch_from):
        move(
            [(sketch_from.at[pl.ds(half, HALF)], sketch)]
            + [
                (pair[which].at[p, sector], ref.at[pl.ds(at, N)])
                for ref, at, which, p, sector in blocks
            ],
            sem,
        )

    pl.when(core == 0)(lambda: load((site, other), mine))
    pl.when(core == 1)(lambda: load((other, site), theirs))
    mask_sketch(sketch, scal)
    for ref, at, which, p, sector in blocks:
        target = wrap(sector + p - (next_step if which else step))
        rows = meta[THERE if which else HERE, 19 + sector]
        cols = meta[AFTER if which else THERE, 19 + target]
        ref[pl.ds(at, N), :] = jnp.where(
            (row < rows) & (col < cols), ref[pl.ds(at, N), :], 0.0
        )
    left[pl.ds(BULK, 8), :] = jnp.ones((8, N), F32)
    right[pl.ds(BULK, 8), :] = jnp.ones((8, N), F32)
    chip[pl.ds(BLOCK, 8), :] = jnp.zeros((8, N), F32)
    cross[pl.ds(BLOCK, 8), :] = jnp.zeros((8, N), F32)


def start(position, meta, site, other, mine, theirs):
    return pl.pallas_call(
        start_kernel,
        out_shape=(
            shape(16),
            shape(16),
            shape(BULK + 8, N),
            shape(BULK + 8, N),
            shape(BLOCK + 8, N),
            shape(BLOCK + 8, N),
            shape(HALF, BLOCK, N),
        ),
        in_specs=[SM, SM, HB, HB, HB, HB],
        out_specs=(SM, SM, VM, VM, VM, VM, VM),
        scratch_shapes=[pltpu.SemaphoreType.DMA((4 * HALF + 5,))],
        compiler_params=pltpu.CompilerParams(vmem_limit_bytes=24 * 1024 * 1024),
        name="start",
    )(position, meta, site, other, mine, theirs)


def odd_sketch_kernel(pos, odd_scal, theirs, behind, sketch, sem):
    core = lax.rem(pos[0], 2)

    def load(source):
        move([(source, sketch)], sem)

    pl.when(core == 0)(lambda: load(theirs.at[pl.ds(0, HALF)]))
    pl.when(core == 1)(lambda: load(behind))
    mask_sketch(sketch, odd_scal)


def odd_sketch(position, odd_scal, theirs, behind):
    return pl.pallas_call(
        odd_sketch_kernel,
        out_shape=shape(HALF, BLOCK, N),
        in_specs=[SM, SM, HB, HB],
        out_specs=VM,
        scratch_shapes=[pltpu.SemaphoreType.DMA((1,))],
        compiler_params=pltpu.CompilerParams(vmem_limit_bytes=16 * 1024 * 1024),
        name="odd_sketch",
    )(position, odd_scal, theirs, behind)


def finish_kernel(pos, meta, recv, swap, out, sem):
    position = pos[0]
    core = lax.rem(position, 2)
    step = jnp.where(core == 0, 0.0, meta[THERE, 6]).astype(jnp.int32)
    sums = recv[pl.ds(BULK, 8), :] + swap[pl.ds(BULK, 8), :]
    weight = sums[0:1, :]

    @pl.when(core == 0)
    def _():
        alpha = 1.0 / jnp.sqrt(weight)
        recv[pl.ds(0, BULK), :] = recv[pl.ds(0, BULK), :] * alpha
        swap[pl.ds(0, BULK), :] = swap[pl.ds(0, BULK), :] * alpha
        pairs = []
        for k in range(HALF):
            for p in range(2):
                rows = pl.ds(k * BLOCK + p * N, N)
                pairs.append((recv.at[rows], out.at[p, k]))
                pairs.append((swap.at[rows], out.at[p, k + HALF]))
        move(pairs, sem)

    @pl.when(core == 1)
    def _():
        pairs = []
        for k in range(HALF):
            for p in range(2):
                rows = pl.ds(k * BLOCK + p * N, N)
                pairs.append((swap.at[rows], out.at[p, wrap(k - p + step)]))
                pairs.append((recv.at[rows], out.at[p, wrap(k + HALF - p + step)]))
        move(pairs, sem)


def finish(position, meta, recv, swap):
    return pl.pallas_call(
        finish_kernel,
        out_shape=shape(2, NSEC, N, N),
        in_specs=[SM, SM, VM, VM],
        out_specs=HB,
        scratch_shapes=[pltpu.SemaphoreType.DMA((4 * HALF,))],
        compiler_params=pltpu.CompilerParams(vmem_limit_bytes=16 * 1024 * 1024),
        name="finish",
    )(position, meta, recv, swap)


def everywhere(value, chain):
    stride = 1
    while stride < chain:
        size = 4 if (chain // stride) % 4 == 0 and stride > 1 else 2
        terms = [value]
        for turn in range(1, size):
            moves = [(i, i ^ (turn * stride)) for i in range(chain)]
            terms.append(lax.ppermute(value, "site", moves))
        while len(terms) > 1:
            terms = [a + b for a, b in zip(terms[0::2], terms[1::2])]
        value = terms[0]
        stride *= size
    return value


def body(sites, sector_sizes, charge_steps, kept_counts, gates, sketches):
    chain = lax.axis_size("site")
    here = lax.axis_index("site").astype(jnp.int32)
    position = jnp.stack([here, jnp.int32(chain)])
    core = here % 2
    chips = chain // 2

    def device(chip, core):
        return 2 * (chip % chips) + core

    swap = [(i, i ^ 1) for i in range(chain)]
    over = [(device(j, 0), device(j + 1, 1)) for j in range(chips)]
    over += [(device(j + 1, 1), device(j, 0)) for j in range(chips)]
    apart = [(device(j, 0), device(j - 1, 0)) for j in range(chips)]
    apart += [(device(j, 1), device(j + 1, 1)) for j in range(chips)]
    back = [(target, source) for source, target in apart]
    slant = [(device(j + 1, 0), device(j, 1)) for j in range(chips)]
    slant += [(device(j, 1), device(j + 1, 0)) for j in range(chips)]
    ahead = [(device(j, 1), device(j + 1, 1)) for j in range(chips)]

    row = jnp.concatenate(
        [
            gates[0],
            charge_steps.astype(F32),
            kept_counts[0].astype(F32),
            sector_sizes[0].astype(F32),
            jnp.zeros((1,), F32),
        ]
    )
    partner = lax.ppermute(row, "site", swap)
    along = lax.ppermute(row, "site", apart)
    across = lax.ppermute(row, "site", slant)
    meta = jnp.stack(
        [
            jnp.where(core == 0, row, partner),
            jnp.where(core == 0, partner, row),
            jnp.where(core == 0, along, across),
            jnp.where(core == 0, across, along),
        ]
    )
    site = sites[0]
    sketch = sketches[0]
    other = lax.ppermute(site, "site", swap)
    theirs = lax.ppermute(sketch, "site", swap)
    later, meta = lax.optimization_barrier((sketch[HALF:], meta))
    behind = lax.ppermute(later, "site", ahead)
    scal, odd_scal, left, right, chip, cross, even = start(
        position, meta, site, other, sketch, theirs
    )
    odd = odd_sketch(position, odd_scal, theirs, behind)

    def spread(out, moves):
        acc, keep, send, chip, cross = out
        recv = lax.ppermute(send, "site", moves)
        cross = lax.ppermute(cross, "site", over)
        chip = lax.ppermute(chip, "site", swap)
        return acc, keep, recv, chip, cross

    none = jnp.zeros((1,), jnp.int32)

    def even_sweep(first, carry):
        return spread(sweep(0, first, scal, *carry, even), apart)

    def odd_sweep(carry):
        return spread(sweep(1, none, odd_scal, *carry, odd), back)

    carry = (jnp.zeros((8, N), F32), left, right, chip, cross)
    carry = even_sweep(none + 1, carry)
    carry = lax.fori_loop(
        0, STEPS - 1, lambda _, carry: even_sweep(none, odd_sweep(carry)), carry
    )
    acc, keep, send, chip, cross = sweep(1, none, odd_scal, *carry, odd)
    tail = keep[BULK:]
    met = tail + lax.ppermute(tail, "site", over)
    weight, total = met[0:1], met[1:2]
    last = jnp.concatenate([1.0 - weight / total, jnp.log(total), met[2:]], axis=0)
    acc = jnp.where(core == 0, acc + last, 0.0)
    totals = everywhere(acc, chain)[0:2, 0]
    recv = lax.ppermute(send, "site", back)
    swapped = lax.ppermute(keep, "site", swap)
    out = finish(position, meta, recv, swapped)
    return (out[None], totals)


def solution(mesh):
    placed = (
        P("site", None, None, None, None),
        P("site", None),
        P("site"),
        P("site", None),
        P("site", None),
        P("site", None, None, None),
    )
    return jax.shard_map(
        body,
        mesh=mesh,
        in_specs=placed,
        out_specs=(P("site", None, None, None, None), P()),
        check_vma=False,
    )
```
